32 devices in a mesh: band: 16 (over z, y, core), spin: 2 (over x).
Axes of the slice: x: 2, y: 2, z: 4, core: 2. Of those that a mesh axis runs over, the one named last changes fastest.
Arguments:
- coefficients: bfloat16 [2, 2, 32, 524288], P('spin', None, 'band'), may hold values from -1 to 1
- occupation: int32 [2, 32], P('spin', 'band'), may hold values from 0 to 1000
- miller: int32 [3, 524288], P(None, ('band', 'spin')), may hold values from -8 to 8
- density: float32 [2, 256, 128, 128], P('spin', 'band'), may hold values from 0.25 to 2
- local_factor: float32 [2, 256, 128, 128], P(None, None, 'band'), may hold values from -1.2 to 1.2
Outputs:
- stress: float32 [6], replicated
- kinetic_density: float32 [524288], P(('band', 'spin'))
- gradient_square: float32 [2, 256, 128, 128], P('spin', 'band')
The draws below stay inside these ranges and needn't reach their ends.
All inputs are finite; a program needn't handle non-finite values.
Results may differ from the reference program's by a relative error of at most 0.0003.
Values sent between devices are 32-bit elements; how exact they have to be, the bound alone decides.
A program may use at most 64 MiB of HBM per device.

```python
import math
import jax
import jax.numpy as jnp
from jax import lax

NPW = 524288
NX = 128
NY = 128
NZ = 256
BANDS = 32
SPINS = 2


def place_ends(result, stream_key, smallest, high):
    longest = result.shape.index(max(result.shape))
    spots = []
    for shift in (0, 1):
        where = [jax.random.randint(jax.random.fold_in(stream_key, axis), (), 0, length) for axis, length in enumerate(result.shape)]
        where[longest] = (where[longest] + shift) % result.shape[longest]
        spots.append(tuple(where))
    return result.at[spots[0]].set(smallest).at[spots[1]].set(high)


def with_spikes(values, rng, source, target, parts, factor):
    def block_of(dim):
        return (jnp.arange(values.shape[dim]) // (values.shape[dim] // parts)).reshape((-1,) + (1,) * (values.ndim - 1 - dim))

    one_side = jax.random.permutation(rng, parts)[block_of(target)]
    other_side = (block_of(target) + parts // 2) % parts
    return jnp.where((block_of(source) == one_side) | (block_of(source) == other_side), factor * values, values)


def steps_of(rng, dims, split, low, largest):
    def one(axis_at, blocks):
        draws = jax.random.uniform(jax.random.fold_in(jax.random.fold_in(rng, 6), axis_at), (blocks,), jnp.float32, low / len(split), largest / len(split))
        return jnp.repeat(jnp.exp(draws), dims[axis_at] // blocks).reshape((-1,) + (1,) * (len(dims) - axis_at - 1))

    level = one(*split[0])
    for cut in split[1:]:
        level = level * one(*cut)
    return level


def bell_draw(rng, dims, deviation, reach, split=(), kind=jnp.bfloat16):
    loudness = steps_of(rng, dims, split, -0.22, 0.18) if split else 1.0
    values = jax.random.normal(rng, dims, jnp.float32) * deviation * loudness
    return jnp.minimum(jnp.maximum(values, -reach), reach).astype(kind)


def heavy_noise(key, shape, width, limit, split, heavy, held_as=jnp.bfloat16):
    entries = width * jax.random.normal(key, shape, jnp.float32)
    if split:
        entries = entries * steps_of(key, shape, split, -0.22, 0.18)
    return jnp.clip(with_spikes(entries, jax.random.fold_in(key, 3), *heavy), -limit, limit).astype(held_as)


def setup_inputs(seed: int = 0) -> dict:
    keys = jax.random.split(jax.random.key(seed), 6)
    coefficients = heavy_noise(keys[0], (SPINS, 2, BANDS, NPW), (2 * BANDS) ** -0.5, 1.0, ((0, 2), (2, 16)), (2, 3, 16, 2.0))
    occupation = place_ends(jax.random.randint(keys[1], (SPINS, BANDS), 0, 1001), jax.random.fold_in(keys[1], 1), 0, 1000).astype(jnp.int32)
    miller = place_ends(jax.random.randint(keys[2], (3, NPW), -8, 9), jax.random.fold_in(keys[2], 1), -8, 8).astype(jnp.int32)
    density = jnp.clip(0.25 + 1.75 * jax.random.uniform(keys[3], (SPINS, NZ, NX, NY), jnp.float32) ** steps_of(keys[3], (SPINS, NZ, NX, NY), ((0, 2), (1, 16)), -0.2, 0.2), 0.25, 2.0)
    local_factor = bell_draw(keys[4], (2, NZ, NX, NY), 0.2, 1.2, ((2, 16),), jnp.float32)
    return {"coefficients": coefficients, "occupation": occupation, "miller": miller, "density": density, "local_factor": local_factor}


occupation_unit = 1000.0
kpoint = (0.25, 0.125, 0.375)
spacing = 0.25


def derivative_table(length):
    row_index = jnp.arange(length, dtype=jnp.int32)[:, None]
    col_index = jnp.arange(length, dtype=jnp.int32)[None, :]
    wrapped = jnp.mod(row_index - col_index, length)
    angles = (jnp.pi / length) * wrapped.astype(jnp.float32)
    on_diagonal = wrapped == 0
    sines = jnp.where(on_diagonal, 1.0, jnp.sin(angles))
    parity = 1.0 - 2.0 * jnp.mod(wrapped, 2).astype(jnp.float32)
    return jnp.where(on_diagonal, 0.0, 0.5 * parity * jnp.cos(angles) / sines).astype(jnp.float32)


def frequencies(length):
    positions = jnp.arange(length, dtype=jnp.int32)
    signed = jnp.where(positions >= length // 2, positions - length, positions)
    return (2.0 * jnp.pi / length) * signed.astype(jnp.float32)


def six_sums(weighting, first_axis, second_axis, third_axis):
    return jnp.stack([
        jnp.sum(weighting * first_axis * first_axis),
        jnp.sum(weighting * second_axis * second_axis),
        jnp.sum(weighting * third_axis * third_axis),
        jnp.sum(weighting * second_axis * third_axis),
        jnp.sum(weighting * first_axis * third_axis),
        jnp.sum(weighting * first_axis * second_axis)])


def reference(coefficients, occupation, miller, density, local_factor):
    highest = lax.Precision.HIGHEST
    weights = occupation.astype(jnp.float32) / occupation_unit
    band_block = math.gcd(BANDS, 32)

    def accumulate(counter, running):
        first_row = (jnp.asarray(counter).astype(jnp.int32) * band_block).astype(jnp.int32)
        piece = lax.dynamic_slice_in_dim(coefficients, first_row, band_block, 2).astype(jnp.float32)
        squares = piece[:, 0] * piece[:, 0] + piece[:, 1] * piece[:, 1]
        weight_piece = lax.dynamic_slice_in_dim(weights, first_row, band_block, 1)
        return running + jnp.einsum('sb,sbg->g', weight_piece, squares, precision=highest)

    kinetic_weight = lax.fori_loop(0, BANDS // band_block, accumulate, jnp.zeros((NPW,), jnp.float32))
    kvec = jnp.array(kpoint, jnp.float32)
    gvec = spacing * (miller.astype(jnp.float32) + kvec[:, None])
    kinetic_density = 0.5 * (gvec[0] ** 2 + gvec[1] ** 2 + gvec[2] ** 2) * kinetic_weight
    kinetic_stress = -six_sums(kinetic_weight, gvec[0], gvec[1], gvec[2]) / NPW

    deriv_x = derivative_table(NX)
    deriv_y = derivative_table(NY)
    deriv_z = derivative_table(NZ)
    grad_x = jnp.einsum('ik,szky->sziy', deriv_x, density, precision=highest)
    grad_y = jnp.einsum('ik,szxk->szxi', deriv_y, density, precision=highest)
    grad_z = jnp.einsum('ik,skxy->sixy', deriv_z, density, precision=highest)
    gradient_square = grad_x * grad_x + grad_y * grad_y + grad_z * grad_z
    kernel = density ** (-1.0 / 3.0) / (1.0 + gradient_square / (4.0 * density * density + 1.0))
    cell_count = NZ * NX * NY
    xc_stress = -six_sums(kernel, grad_x, grad_y, grad_z) / cell_count

    total_density = jnp.sum(density, axis=0)
    spectrum = jnp.fft.fftn(total_density) / cell_count
    real_part = jnp.real(spectrum)
    imag_part = jnp.imag(spectrum)
    freq_z = frequencies(NZ)[:, None, None]
    freq_x = frequencies(NX)[None, :, None]
    freq_y = frequencies(NY)[None, None, :]
    length_sq = freq_x * freq_x + freq_y * freq_y + freq_z * freq_z
    positive = length_sq > 0
    inverse = jnp.where(positive, 1.0 / jnp.where(positive, length_sq, 1.0), 0.0)
    hartree_weight = 4.0 * jnp.pi * (real_part * real_part + imag_part * imag_part) * inverse
    diagonal = jnp.array([1.0, 1.0, 1.0, 0.0, 0.0, 0.0], jnp.float32)
    hartree_stress = 2.0 * six_sums(hartree_weight * inverse, freq_x, freq_y, freq_z) - diagonal * jnp.sum(hartree_weight)
    local_weight = 2.0 * (real_part * local_factor[0] + imag_part * local_factor[1])
    local_stress = six_sums(local_weight, freq_x, freq_y, freq_z)
    stress = kinetic_stress + hartree_stress + local_stress + xc_stress
    return stress, kinetic_density, gradient_square
```

```python
import functools

import jax
import jax.numpy as jnp
import numpy as np
from jax import lax
from jax.experimental import pallas as pl
from jax.experimental.pallas import tpu as pltpu
from jax.sharding import PartitionSpec as P

occupation_unit = 1000.0
kpoint = (0.25, 0.125, 0.375)
spacing = 0.25
MESH = pl.DeviceIdType.MESH
VMEM = pl.BlockSpec(memory_space=pltpu.VMEM)


def derivative_table(length):
    index = np.arange(length)
    wrapped = np.mod(index[:, None] - index[None, :], length)
    angles = np.pi / length * wrapped
    sines = np.where(wrapped == 0, 1.0, np.sin(angles))
    parity = 1.0 - 2.0 * np.mod(wrapped, 2)
    table = np.where(wrapped == 0, 0.0, 0.5 * parity * np.cos(angles) / sines)
    return table.astype(np.float32)


def fourier_tables(length):
    index = np.arange(length)
    phases = np.mod(index[:, None] * index[None, :], length) * (2.0 * np.pi / length)
    return np.cos(phases), np.sin(phases)


def frequencies(length):
    index = np.arange(length)
    signed = np.where(index >= length // 2, index - length, index)
    return (2.0 * np.pi / length * signed).astype(np.float32)


def six_rows(weighting, first_axis, second_axis, third_axis):
    dims = tuple(range(weighting.ndim - 1))
    wx, wy, wz = weighting * first_axis, weighting * second_axis, weighting * third_axis
    terms = (
        wx * first_axis,
        wy * second_axis,
        wz * third_axis,
        wy * third_axis,
        wx * third_axis,
        wx * second_axis,
    )
    return jnp.stack([jnp.sum(t, axis=dims) for t in terms])


def greet_all(nb, ns):
    b, s = lax.axis_index("band"), lax.axis_index("spin")
    barrier = pltpu.get_barrier_semaphore()

    def greet(k, carry):
        pl.semaphore_signal(
            barrier,
            inc=1,
            device_id=((b + k // ns) % nb, (s + k % ns) % ns),
            device_id_type=MESH,
        )
        return carry

    lax.fori_loop(1, nb * ns, greet, 0)
    pl.semaphore_wait(barrier, nb * ns - 1)
    return b, s


def far_first(k, count):
    return 1 + (k + count // 2 - 1) % (count - 1)


def first_kernel(
    nb, ns, ny, nz, dens, kin, dcol, half, kout,
    from_core, sum_core, from_plane, sum_plane, from_line,
    d_send, d_recv, h_send, h_recv, c_send, c_recv, p_send, p_recv, l_send, l_recv,
):
    b, s = greet_all(nb, ns)
    core, y, z = b % 2, (b // 2) % ny, b // (2 * ny)
    zh = dens.shape[0] // ns

    core_copy = pltpu.make_async_remote_copy(
        kin.at[:, :, 1 - core], from_core, c_send.at[0], c_recv.at[0],
        device_id=(b + 1 - 2 * core, s), device_id_type=MESH,
    )
    core_copy.start()

    half_copies = []
    for k in range(1, ns):
        other = (s + k) % ns
        half_copies.append(
            pltpu.make_async_remote_copy(
                dens.at[pl.ds(other * zh, zh)], half.at[k - 1], h_send.at[k - 1], h_recv.at[k - 1],
                device_id=(b, other), device_id_type=MESH,
            )
        )

    def column_copy(k):
        offset = far_first(k, nb)
        to = (b + offset) % nb
        return pltpu.make_async_remote_copy(
            dens.at[:, to], dcol.at[b], d_send.at[k], d_recv.at[k],
            device_id=(to, s), device_id_type=MESH,
        )

    def start_column(k, carry):
        column_copy(k).start()
        return carry

    lax.fori_loop(0, nb - 1, start_column, 0)
    for copy in half_copies:
        copy.start()
    dcol[b] = dens[:, b]

    core_copy.wait()
    sum_core[...] = kin[:, :, core] + from_core[...]
    plane_copies = []
    for k in range(1, ny * ns):
        ty, ts = (y + k // ns) % ny, (s + k % ns) % ns
        copy = pltpu.make_async_remote_copy(
            sum_core.at[:, ty, ts], from_plane.at[k - 1], p_send.at[k - 1], p_recv.at[k - 1],
            device_id=((z * ny + ty) * 2 + core, ts), device_id_type=MESH,
        )
        copy.start()
        plane_copies.append(copy)
    for copy in plane_copies:
        copy.wait()
    total = sum_core[:, y, s]
    for k in range(1, ny * ns):
        total = total + from_plane[k - 1]
    sum_plane[...] = total

    def line_copy(k):
        tz = (z + k) % nz
        return pltpu.make_async_remote_copy(
            sum_plane.at[tz], from_line.at[k - 1], l_send.at[k - 1], l_recv.at[k - 1],
            device_id=((tz * ny + y) * 2 + core, s), device_id_type=MESH,
        )

    def start_line(k, carry):
        line_copy(k).start()
        return carry

    def wait_line(k, carry):
        line_copy(k).wait()
        return carry

    lax.fori_loop(1, nz, start_line, 0)
    lax.fori_loop(1, nz, wait_line, 0)
    kout[...] = sum_plane[z] + jnp.sum(from_line[...], axis=0)

    for copy in half_copies:
        copy.wait()

    def wait_column(k, carry):
        column_copy(k).wait()
        return carry

    lax.fori_loop(0, nb - 1, wait_column, 0)


def second_kernel(nb, ns, spec, grad, scol, gout, s_send, s_recv, g_send, g_recv):
    b, s = greet_all(nb, ns)
    n = nb * ns

    def spec_copy(k):
        offset = far_first(k, n)
        tb, ts = (b + offset // ns) % nb, (s + offset % ns) % ns
        return pltpu.make_async_remote_copy(
            spec.at[ts, :, tb], scol.at[b, s], s_send.at[k], s_recv.at[k],
            device_id=(tb, ts), device_id_type=MESH,
        )

    def grad_copy(k):
        to = (b + far_first(k, nb)) % nb
        return pltpu.make_async_remote_copy(
            grad.at[to], gout.at[:, b], g_send.at[k], g_recv.at[k],
            device_id=(to, s), device_id_type=MESH,
        )

    def start_grad(k, carry):
        grad_copy(k).start()
        return carry

    def start_spec(k, carry):
        spec_copy(k).start()
        return carry

    lax.fori_loop(0, nb - 1, start_grad, 0)
    lax.fori_loop(0, n - 1, start_spec, 0)
    gout[:, b] = grad[b]
    scol[b, s] = spec[s, :, b]

    def wait_grad(k, carry):
        grad_copy(k).wait()
        return carry

    def wait_spec(k, carry):
        spec_copy(k).wait()
        return carry

    lax.fori_loop(0, nb - 1, wait_grad, 0)
    lax.fori_loop(0, n - 1, wait_spec, 0)


def third_kernel(nb, ns, part, out, held, send, recv):
    b, s = greet_all(nb, ns)
    n = nb * ns

    def copy_of(k):
        tb, ts = (b + k // ns) % nb, (s + k % ns) % ns
        return pltpu.make_async_remote_copy(
            part, held.at[k - 1], send.at[k - 1], recv.at[k - 1],
            device_id=(tb, ts), device_id_type=MESH,
        )

    def start(k, carry):
        copy_of(k).start()
        return carry

    def wait(k, carry):
        copy_of(k).wait()
        return carry

    lax.fori_loop(1, n, start, 0)
    lax.fori_loop(1, n, wait, 0)
    out[...] = part[...] + jnp.sum(held[...], axis=0)


def params(number):
    return pltpu.CompilerParams(
        collective_id=number, has_side_effects=True, vmem_limit_bytes=40 * 2**20
    )


def f32(*shape):
    return jax.ShapeDtypeStruct(shape, jnp.float32)


def shards(nb, ns, coefficients, occupation, miller, density, local_factor):
    high = lax.Precision.HIGH
    dma = pltpu.SemaphoreType.DMA
    _, zl, nx, ny = density.shape
    nzg = zl * nb
    xl = nx // nb
    zh = zl // ns
    lanes = 2 * ny // ns
    cells = nzg * nx * ny
    npw = coefficients.shape[3]
    rows = npw // (nb * ns * 128)
    fold_y = 2 if nb % 4 == 0 else 1
    fold_z = nb // (2 * fold_y)
    b, s = lax.axis_index("band"), lax.axis_index("spin")

    weights = occupation[0].astype(jnp.float32) / occupation_unit
    piece = coefficients[0].astype(jnp.float32)
    kin = jnp.sum(weights[:, None] * (piece[0] * piece[0] + piece[1] * piece[1]), axis=0)
    kin = kin.reshape(fold_z, fold_y, 2, ns, rows, 128)
    dens = density[0]

    dcol, half, kinetic_weight = pl.pallas_call(
        functools.partial(first_kernel, nb, ns, fold_y, fold_z),
        out_shape=(f32(nb, zl, xl, ny), f32(ns - 1, zh, nb, xl, ny), f32(rows, 128)),
        in_specs=[VMEM] * 2,
        out_specs=(VMEM,) * 3,
        scratch_shapes=[
            pltpu.VMEM((fold_z, fold_y, ns, rows, 128), jnp.float32),
            pltpu.VMEM((fold_z, fold_y, ns, rows, 128), jnp.float32),
            pltpu.VMEM((fold_y * ns - 1, fold_z, rows, 128), jnp.float32),
            pltpu.VMEM((fold_z, rows, 128), jnp.float32),
            pltpu.VMEM((fold_z - 1, rows, 128), jnp.float32),
            dma((nb - 1,)), dma((nb - 1,)), dma((ns - 1,)), dma((ns - 1,)), dma((1,)), dma((1,)),
            dma((fold_y * ns - 1,)), dma((fold_y * ns - 1,)), dma((fold_z - 1,)), dma((fold_z - 1,)),
        ],
        compiler_params=params(0),
        name="first_exchange",
    )(dens.reshape(zl, nb, xl, ny), kin)

    own = lax.dynamic_slice_in_dim(dens, s * zh, zh, 0)
    total = own + jnp.sum(half, axis=0).reshape(zh, nx, ny)
    cos_x, sin_x = fourier_tables(nx)
    cos_y, sin_y = fourier_tables(ny)
    cos_z, sin_z = fourier_tables(nzg)
    along = jnp.concatenate(
        [
            jnp.einsum("mj,zjy->zmy", cos_x.astype(np.float32), total, precision=high),
            jnp.einsum("mj,zjy->zmy", (-sin_x).astype(np.float32), total, precision=high),
        ],
        axis=2,
    ).reshape(zh * nx, 2 * ny)
    part = ny // ns
    planes = []
    for k in range(ns):
        cut = slice(k * part, (k + 1) * part)
        table = np.block([[cos_y[:, cut], -sin_y[:, cut]], [sin_y[:, cut], cos_y[:, cut]]])
        planes.append(jnp.dot(along, table.astype(np.float32), precision=high))
    spec = jnp.stack(planes).reshape(ns, zh, nb, xl, lanes)

    grad_col = jnp.dot(derivative_table(nzg), dcol.reshape(nzg, xl * ny), precision=high)

    scol, gout = pl.pallas_call(
        functools.partial(second_kernel, nb, ns),
        out_shape=(f32(nb, ns, zh, xl, lanes), f32(zl, nb, xl, ny)),
        in_specs=[VMEM] * 2,
        out_specs=(VMEM,) * 2,
        scratch_shapes=[
            dma((nb * ns - 1,)), dma((nb * ns - 1,)), dma((nb - 1,)), dma((nb - 1,)),
        ],
        compiler_params=params(1),
        name="second_exchange",
    )(spec, grad_col.reshape(nb, zl, xl, ny))

    gvec = spacing * (miller.astype(jnp.float32) + jnp.array(kpoint, jnp.float32)[:, None])
    gvec = gvec.reshape(3, rows, 128)
    kinetic_density = (
        0.5 * (gvec[0] ** 2 + gvec[1] ** 2 + gvec[2] ** 2) * kinetic_weight
    ).reshape(rows * 128)
    stress_rows = -six_rows(kinetic_weight, gvec[0], gvec[1], gvec[2]) / npw

    grad_x = jnp.einsum("ik,zky->ziy", derivative_table(nx), dens, precision=high)
    grad_y = jnp.einsum("ik,zxk->zxi", derivative_table(ny), dens, precision=high)
    grad_z = gout.reshape(zl, nx, ny)
    square = grad_x * grad_x + grad_y * grad_y + grad_z * grad_z
    kernel = dens ** (-1.0 / 3.0) / (1.0 + square / (4.0 * dens * dens + 1.0))
    stress_rows = stress_rows - six_rows(kernel, grad_x, grad_y, grad_z) / cells

    tables = (np.concatenate([cos_z, sin_z]) / cells).astype(np.float32)
    turned = jnp.dot(tables, scol.reshape(nzg, xl * lanes), precision=high)
    turned = turned.reshape(2, nzg, xl, lanes)
    real = turned[0, :, :, :part] + turned[1, :, :, part:]
    imag = turned[0, :, :, part:] - turned[1, :, :, :part]
    spectrum = jnp.concatenate([real, imag], axis=2)
    factor = lax.dynamic_slice_in_dim(local_factor, s * part, part, 3)
    factor = jnp.concatenate([factor[0], factor[1]], axis=2)
    freq_z = frequencies(nzg)[:, None, None]
    freq_x = lax.dynamic_slice_in_dim(jnp.asarray(frequencies(nx)), b * xl, xl, 0)[None, :, None]
    freq_y = lax.dynamic_slice_in_dim(jnp.asarray(frequencies(ny)), s * part, part, 0)
    freq_y = jnp.concatenate([freq_y, freq_y])[None, None, :]
    length_sq = freq_x * freq_x + freq_y * freq_y + freq_z * freq_z
    positive = length_sq > 0
    inverse = jnp.where(positive, 1.0 / jnp.where(positive, length_sq, 1.0), 0.0)
    hartree = 4.0 * jnp.pi * spectrum * spectrum * inverse
    weight = 2.0 * (hartree * inverse + spectrum * factor)
    spec_rows = six_rows(weight, freq_x, freq_y, freq_z)
    diagonal = np.array([1.0, 1.0, 1.0, 0.0, 0.0, 0.0], np.float32)[:, None]
    spec_rows = spec_rows - diagonal * jnp.sum(hartree, axis=(0, 1))[None]
    stress_rows = stress_rows + spec_rows

    stress = pl.pallas_call(
        functools.partial(third_kernel, nb, ns),
        out_shape=f32(8, 128),
        in_specs=[VMEM],
        out_specs=VMEM,
        scratch_shapes=[
            pltpu.VMEM((nb * ns - 1, 8, 128), jnp.float32),
            dma((nb * ns - 1,)), dma((nb * ns - 1,)),
        ],
        compiler_params=params(2),
        name="stress_sum",
    )(jnp.concatenate([stress_rows, jnp.zeros((2, 128), jnp.float32)]))
    return (jnp.sum(stress[:6], axis=1), kinetic_density, square[None])


def solution(mesh):
    return jax.shard_map(
        functools.partial(shards, mesh.shape["band"], mesh.shape["spin"]),
        mesh=mesh,
        in_specs=(
            P("spin", None, "band", None),
            P("spin", "band"),
            P(None, ("band", "spin")),
            P("spin", "band", None, None),
            P(None, None, "band", None),
        ),
        out_specs=(P(), P(("band", "spin")), P("spin", "band", None, None)),
        check_vma=False,
    )
```

```python
import functools

import jax
import jax.numpy as jnp
import numpy as np
from jax import lax
from jax.experimental import pallas as pl
from jax.experimental.pallas import tpu as pltpu
from jax.sharding import PartitionSpec as P

occupation_unit = 1000.0
kpoint = (0.25, 0.125, 0.375)
spacing = 0.25
MESH = pl.DeviceIdType.MESH
VMEM = pl.BlockSpec(memory_space=pltpu.VMEM)


def derivative_table(length):
    index = np.arange(length)
    wrapped = np.mod(index[:, None] - index[None, :], length)
    angles = np.pi / length * wrapped
    sines = np.where(wrapped == 0, 1.0, np.sin(angles))
    parity = 1.0 - 2.0 * np.mod(wrapped, 2)
    table = np.where(wrapped == 0, 0.0, 0.5 * parity * np.cos(angles) / sines)
    return table.astype(np.float32)


def fourier_tables(length):
    index = np.arange(length)
    phases = np.mod(index[:, None] * index[None, :], length) * (2.0 * np.pi / length)
    return np.cos(phases), np.sin(phases)


def frequencies(length):
    index = np.arange(length)
    signed = np.where(index >= length // 2, index - length, index)
    return (2.0 * np.pi / length * signed).astype(np.float32)


def six_rows(weighting, first_axis, second_axis, third_axis):
    dims = tuple(range(weighting.ndim - 1))
    wx, wy, wz = weighting * first_axis, weighting * second_axis, weighting * third_axis
    terms = (
        wx * first_axis,
        wy * second_axis,
        wz * third_axis,
        wy * third_axis,
        wx * third_axis,
        wx * second_axis,
    )
    return jnp.stack([jnp.sum(t, axis=dims) for t in terms])


def greet_all(nb, ns):
    b, s = lax.axis_index("band"), lax.axis_index("spin")
    barrier = pltpu.get_barrier_semaphore()

    def greet(k, carry):
        pl.semaphore_signal(
            barrier,
            inc=1,
            device_id=((b + k // ns) % nb, (s + k % ns) % ns),
            device_id_type=MESH,
        )
        return carry

    lax.fori_loop(1, nb * ns, greet, 0)
    pl.semaphore_wait(barrier, nb * ns - 1)
    return b, s


def far_first(k, count):
    return 1 + (k + count // 2 - 1) % (count - 1)


def split(value):
    high = value.astype(jnp.bfloat16)
    return high, (value - high.astype(jnp.float32)).astype(jnp.bfloat16)


def host_split(table):
    high = table.astype(np.float32).astype(jnp.bfloat16)
    low = (table - high.astype(np.float64)).astype(np.float32).astype(jnp.bfloat16)
    return np.stack([high, low])


def dot3(left, right):
    def one(p, q):
        return jnp.dot(p, q, preferred_element_type=jnp.float32)

    return one(left[0], right[0]) + (one(left[0], right[1]) + one(left[1], right[0]))


def loop(low, high, step):
    def body(k, carry):
        step(k)
        return carry

    lax.fori_loop(low, high, body, 0)


def main_kernel(
    nb, ns, ny, nz, dens, coef, weight, pairs, table_x, table_y, table_d,
    scol, gout, kout,
    kin, dcol, half, spec, grad, from_core, sum_core, from_plane, sum_plane, from_line,
    d_send, d_recv, h_send, h_recv, c_send, c_recv, p_send, p_recv, l_send, l_recv,
    s_send, s_recv, g_send, g_recv,
):
    b, s = greet_all(nb, ns)
    n = nb * ns
    core, y, z = b % 2, (b // 2) % ny, b // (2 * ny)
    zl, _, xl, width = dens.shape
    zh = zl // ns
    nx = nb * xl
    rows = kout.shape[0]

    half_copies = []
    for k in range(1, ns):
        other = (s + k) % ns
        copy = pltpu.make_async_remote_copy(
            dens.at[pl.ds(other * zh, zh)], half.at[k - 1], h_send.at[k - 1], h_recv.at[k - 1],
            device_id=(b, other), device_id_type=MESH,
        )
        copy.start()
        half_copies.append(copy)

    def column_copy(k):
        to = (b + far_first(k, nb)) % nb
        return pltpu.make_async_remote_copy(
            dens.at[:, to], dcol.at[b], d_send.at[k], d_recv.at[k],
            device_id=(to, s), device_id_type=MESH,
        )

    loop(0, nb - 1, lambda k: column_copy(k).start())
    dcol[b] = dens[:, b]

    depth = weight.shape[0]

    def kinetic(i):
        here = pl.ds(pl.multiple_of(i * depth, depth), depth)
        real, imag = coef[0, here, :].astype(jnp.float32), coef[1, here, :].astype(jnp.float32)
        high, low = split(weight[...] * (real * real + imag * imag))
        kin[i // (2 * ns), (i // ns) % 2, i % ns] = jnp.dot(
            pairs[...], high, preferred_element_type=jnp.float32
        ) + jnp.dot(pairs[...], low, preferred_element_type=jnp.float32)

    loop(0, n, kinetic)
    core_copy = pltpu.make_async_remote_copy(
        kin.at[:, 1 - core], from_core, c_send.at[0], c_recv.at[0],
        device_id=(b + 1 - 2 * core, s), device_id_type=MESH,
    )
    core_copy.start()
    core_copy.wait()

    def add_core(i):
        sum_core[i // ny, i % ny] = kin[i, core] + from_core[i]

    loop(0, nz * ny, add_core)
    plane_copies = []
    for k in range(1, ny * ns):
        ty, ts = (y + k // ns) % ny, (s + k % ns) % ns
        copy = pltpu.make_async_remote_copy(
            sum_core.at[:, ty, ts], from_plane.at[k - 1], p_send.at[k - 1], p_recv.at[k - 1],
            device_id=((z * ny + ty) * 2 + core, ts), device_id_type=MESH,
        )
        copy.start()
        plane_copies.append(copy)

    for copy in half_copies:
        copy.wait()

    def plane(i):
        total = dens[s * zh + i]
        for k in range(ns - 1):
            total = total + half[k, i]
        along = dot3((table_x[0], table_x[1]), split(total.reshape(nx, width)))
        both = split(jnp.concatenate([along[:nx], along[nx:]], axis=1))
        for k in range(ns):
            spec[k, i] = dot3(both, (table_y[0, k], table_y[1, k])).reshape(nb, xl, -1)

    loop(0, zh, plane)

    def spec_copy(k):
        offset = far_first(k, n)
        tb, ts = (b + offset // ns) % nb, (s + offset % ns) % ns
        return pltpu.make_async_remote_copy(
            spec.at[ts, :, tb], scol.at[b, s], s_send.at[k], s_recv.at[k],
            device_id=(tb, ts), device_id_type=MESH,
        )

    loop(0, n - 1, lambda k: spec_copy(k).start())
    scol[b, s] = spec[s, :, b]

    loop(0, nb - 1, lambda k: column_copy(k).wait())
    for x in range(xl):
        column = split(dcol[:, :, x, :].reshape(nb * zl, width))
        grad[:, :, x, :] = dot3((table_d[0], table_d[1]), column).reshape(nb, zl, width)

    def grad_copy(k):
        to = (b + far_first(k, nb)) % nb
        return pltpu.make_async_remote_copy(
            grad.at[to], gout.at[:, b], g_send.at[k], g_recv.at[k],
            device_id=(to, s), device_id_type=MESH,
        )

    loop(0, nb - 1, lambda k: grad_copy(k).start())
    gout[:, b] = grad[b]

    for copy in plane_copies:
        copy.wait()
    total = sum_core[:, y, s]
    for k in range(1, ny * ns):
        total = total + from_plane[k - 1]
    sum_plane[...] = total

    def line_copy(k):
        tz = (z + k) % nz
        return pltpu.make_async_remote_copy(
            sum_plane.at[tz], from_line.at[k - 1], l_send.at[k - 1], l_recv.at[k - 1],
            device_id=((tz * ny + y) * 2 + core, s), device_id_type=MESH,
        )

    loop(1, nz, lambda k: line_copy(k).start())
    loop(1, nz, lambda k: line_copy(k).wait())
    kout[...] = sum_plane[z] + jnp.sum(from_line[...], axis=0)
    loop(0, n - 1, lambda k: spec_copy(k).wait())
    loop(0, nb - 1, lambda k: grad_copy(k).wait())


def third_kernel(nb, ns, part, out, held, send, recv):
    b, s = greet_all(nb, ns)
    n = nb * ns

    def copy_of(k):
        tb, ts = (b + k // ns) % nb, (s + k % ns) % ns
        return pltpu.make_async_remote_copy(
            part, held.at[k - 1], send.at[k - 1], recv.at[k - 1],
            device_id=(tb, ts), device_id_type=MESH,
        )

    def start(k, carry):
        copy_of(k).start()
        return carry

    def wait(k, carry):
        copy_of(k).wait()
        return carry

    lax.fori_loop(1, n, start, 0)
    lax.fori_loop(1, n, wait, 0)
    out[...] = part[...] + jnp.sum(held[...], axis=0)


def params(number):
    return pltpu.CompilerParams(
        collective_id=number, has_side_effects=True, vmem_limit_bytes=40 * 2**20
    )


def f32(*shape):
    return jax.ShapeDtypeStruct(shape, jnp.float32)


def shards(nb, ns, coefficients, occupation, miller, density, local_factor):
    high = lax.Precision.HIGH
    dma = pltpu.SemaphoreType.DMA
    _, zl, nx, ny = density.shape
    nzg = zl * nb
    xl = nx // nb
    zh = zl // ns
    lanes = 2 * ny // ns
    cells = nzg * nx * ny
    npw = coefficients.shape[3]
    rows = npw // (nb * ns * 128)
    fold_y = 2 if nb % 4 == 0 else 1
    fold_z = nb // (2 * fold_y)
    b, s = lax.axis_index("band"), lax.axis_index("spin")

    weights = occupation[0].astype(jnp.float32) / occupation_unit
    nbl = coefficients.shape[2]
    depth = rows * nbl
    coef = coefficients[0].reshape(2, nbl, npw // 128, 128)
    coef = coef.transpose(0, 2, 1, 3).reshape(2, npw // 128 * nbl, 128)
    weight = jnp.broadcast_to(jnp.tile(weights, rows)[:, None], (depth, 128))
    pairs = jnp.asarray(np.kron(np.eye(rows), np.ones((1, nbl))), jnp.bfloat16)
    dens = density[0]
    cos_x, sin_x = fourier_tables(nx)
    cos_y, sin_y = fourier_tables(ny)
    cos_z, sin_z = fourier_tables(nzg)
    part = ny // ns
    table_y = []
    for k in range(ns):
        cut = slice(k * part, (k + 1) * part)
        table_y.append(np.block([[cos_y[:, cut], -sin_y[:, cut]], [sin_y[:, cut], cos_y[:, cut]]]))

    scol, gout, kinetic_weight = pl.pallas_call(
        functools.partial(main_kernel, nb, ns, fold_y, fold_z),
        out_shape=(f32(nb, ns, zh, xl, lanes), f32(zl, nb, xl, ny), f32(rows, 128)),
        in_specs=[VMEM] * 7,
        out_specs=(VMEM,) * 3,
        scratch_shapes=[
            pltpu.VMEM(shape, jnp.float32)
            for shape in (
                (fold_z * fold_y, 2, ns, rows, 128),
                (nb, zl, xl, ny),
                (ns - 1, zh, nb, xl, ny),
                (ns, zh, nb, xl, lanes),
                (nb, zl, xl, ny),
                (fold_z * fold_y, ns, rows, 128),
                (fold_z, fold_y, ns, rows, 128),
                (fold_y * ns - 1, fold_z, rows, 128),
                (fold_z, rows, 128),
                (fold_z - 1, rows, 128),
            )
        ]
        + [
            dma((count,))
            for length in (nb - 1, ns - 1, 1, fold_y * ns - 1, fold_z - 1, nb * ns - 1, nb - 1)
            for count in (length, length)
        ],
        compiler_params=params(0),
        name="main_exchange",
    )(
        dens.reshape(zl, nb, xl, ny),
        coef,
        weight,
        pairs,
        host_split(np.concatenate([cos_x, -sin_x])),
        host_split(np.stack(table_y)),
        host_split(derivative_table(nzg).astype(np.float64)),
    )

    gvec = spacing * (miller.astype(jnp.float32) + jnp.array(kpoint, jnp.float32)[:, None])
    gvec = gvec.reshape(3, rows, 128)
    kinetic_density = (
        0.5 * (gvec[0] ** 2 + gvec[1] ** 2 + gvec[2] ** 2) * kinetic_weight
    ).reshape(rows * 128)
    stress_rows = -six_rows(kinetic_weight, gvec[0], gvec[1], gvec[2]) / npw

    grad_x = jnp.einsum("ik,zky->ziy", derivative_table(nx), dens, precision=high)
    grad_y = jnp.einsum("ik,zxk->zxi", derivative_table(ny), dens, precision=high)
    grad_z = gout.reshape(zl, nx, ny)
    square = grad_x * grad_x + grad_y * grad_y + grad_z * grad_z
    kernel = dens ** (-1.0 / 3.0) / (1.0 + square / (4.0 * dens * dens + 1.0))
    stress_rows = stress_rows - six_rows(kernel, grad_x, grad_y, grad_z) / cells

    tables = (np.concatenate([cos_z, sin_z]) / cells).astype(np.float32)
    turned = jnp.dot(tables, scol.reshape(nzg, xl * lanes), precision=high)
    turned = turned.reshape(2, nzg, xl, lanes)
    real = turned[0, :, :, :part] + turned[1, :, :, part:]
    imag = turned[0, :, :, part:] - turned[1, :, :, :part]
    spectrum = jnp.concatenate([real, imag], axis=2)
    factor = lax.dynamic_slice_in_dim(local_factor, s * part, part, 3)
    factor = jnp.concatenate([factor[0], factor[1]], axis=2)
    freq_z = frequencies(nzg)[:, None, None]
    freq_x = lax.dynamic_slice_in_dim(jnp.asarray(frequencies(nx)), b * xl, xl, 0)[None, :, None]
    freq_y = lax.dynamic_slice_in_dim(jnp.asarray(frequencies(ny)), s * part, part, 0)
    freq_y = jnp.concatenate([freq_y, freq_y])[None, None, :]
    length_sq = freq_x * freq_x + freq_y * freq_y + freq_z * freq_z
    positive = length_sq > 0
    inverse = jnp.where(positive, 1.0 / jnp.where(positive, length_sq, 1.0), 0.0)
    hartree = 4.0 * jnp.pi * spectrum * spectrum * inverse
    weight = 2.0 * (hartree * inverse + spectrum * factor)
    spec_rows = six_rows(weight, freq_x, freq_y, freq_z)
    diagonal = np.array([1.0, 1.0, 1.0, 0.0, 0.0, 0.0], np.float32)[:, None]
    spec_rows = spec_rows - diagonal * jnp.sum(hartree, axis=(0, 1))[None]
    stress_rows = stress_rows + spec_rows

    stress = pl.pallas_call(
        functools.partial(third_kernel, nb, ns),
        out_shape=f32(8, 128),
        in_specs=[VMEM],
        out_specs=VMEM,
        scratch_shapes=[
            pltpu.VMEM((nb * ns - 1, 8, 128), jnp.float32),
            dma((nb * ns - 1,)), dma((nb * ns - 1,)),
        ],
        compiler_params=params(2),
        name="stress_sum",
    )(jnp.concatenate([stress_rows, jnp.zeros((2, 128), jnp.float32)]))
    return (jnp.sum(stress[:6], axis=1), kinetic_density, square[None])


def solution(mesh):
    return jax.shard_map(
        functools.partial(shards, mesh.shape["band"], mesh.shape["spin"]),
        mesh=mesh,
        in_specs=(
            P("spin", None, "band", None),
            P("spin", "band"),
            P(None, ("band", "spin")),
            P("spin", "band", None, None),
            P(None, None, "band", None),
        ),
        out_specs=(P(), P(("band", "spin")), P("spin", "band", None, None)),
        check_vma=False,
    )
```

```python
import functools

import jax
import jax.numpy as jnp
import numpy as np
from jax import lax
from jax.experimental import pallas as pl
from jax.experimental.pallas import tpu as pltpu
from jax.sharding import PartitionSpec as P

occupation_unit = 1000.0
kpoint = (0.25, 0.125, 0.375)
spacing = 0.25
MESH = pl.DeviceIdType.MESH
VMEM = pl.BlockSpec(memory_space=pltpu.VMEM)


def derivative_table(length):
    index = np.arange(length)
    wrapped = np.mod(index[:, None] - index[None, :], length)
    angles = np.pi / length * wrapped
    sines = np.where(wrapped == 0, 1.0, np.sin(angles))
    parity = 1.0 - 2.0 * np.mod(wrapped, 2)
    table = np.where(wrapped == 0, 0.0, 0.5 * parity * np.cos(angles) / sines)
    return table.astype(np.float32)


def fourier_tables(length):
    index = np.arange(length)
    phases = np.mod(index[:, None] * index[None, :], length) * (2.0 * np.pi / length)
    return np.cos(phases), np.sin(phases)


def greet_all(nb, ns):
    b, s = lax.axis_index("band"), lax.axis_index("spin")
    barrier = pltpu.get_barrier_semaphore()

    def greet(k, carry):
        pl.semaphore_signal(
            barrier,
            inc=1,
            device_id=((b + k // ns) % nb, (s + k % ns) % ns),
            device_id_type=MESH,
        )
        return carry

    lax.fori_loop(1, nb * ns, greet, 0)
    pl.semaphore_wait(barrier, nb * ns - 1)
    return b, s


def far_first(k, count):
    return 1 + (k + count // 2 - 1) % (count - 1)


def split(value):
    high = value.astype(jnp.bfloat16)
    return high, (value - high.astype(jnp.float32)).astype(jnp.bfloat16)


def host_split(table):
    high = table.astype(np.float32).astype(jnp.bfloat16)
    low = (table - high.astype(np.float64)).astype(np.float32).astype(jnp.bfloat16)
    return np.stack([high, low])


def dot3(left, right):
    def one(p, q):
        return jnp.dot(p, q, preferred_element_type=jnp.float32)

    return one(left[0], right[0]) + (one(left[0], right[1]) + one(left[1], right[0]))


def loop(low, high, step):
    def body(k, carry):
        step(k)
        return carry

    lax.fori_loop(low, high, body, 0)


def axis_frequency(index, length):
    signed = jnp.where(index >= length // 2, index - length, index)
    return 2.0 * np.pi / length * signed.astype(jnp.float32)


def fold(value):
    return jnp.sum(value, axis=0, keepdims=True)


def main_kernel(
    nb, ns, ny, nz, occupation, miller, dens_h, coef_h, factor_h,
    table_x_h, table_y_h, table_d_h, table_z_h, table_g_h, pairs_h,
    stress, kdens, square,
    dens, coef, factor, table_x, table_y, table_d, table_z, table_g, pairs,
    kin, dcol, half, spec, grad, from_core, sum_core, from_plane, sum_plane, from_line,
    scol, gout, grad_x, grad_y, part, held,
    f_sem, d_send, d_recv, h_send, h_recv, c_send, c_recv, p_send, p_recv, l_send, l_recv,
    s_send, s_recv, g_send, g_recv, t_send, t_recv,
):
    sources = (dens_h, coef_h, pairs_h, table_x_h, table_y_h, table_g_h, table_d_h, table_z_h, factor_h)
    targets = (dens, coef, pairs, table_x, table_y, table_g, table_d, table_z, factor)
    fetches = [
        pltpu.make_async_copy(source, target, f_sem.at[i])
        for i, (source, target) in enumerate(zip(sources, targets))
    ]
    for fetch in fetches:
        fetch.start()
    b, s = greet_all(nb, ns)
    n = nb * ns
    core, y, z = b % 2, (b // 2) % ny, b // (2 * ny)
    zl, _, xl, width = dens.shape
    zh = zl // ns
    nx = nb * xl
    nzg = nb * zl
    rows = kdens.shape[0]
    fetches[0].wait()

    half_copies = []
    for k in range(1, ns):
        other = (s + k) % ns
        copy = pltpu.make_async_remote_copy(
            dens.at[pl.ds(other * zh, zh)], half.at[k - 1], h_send.at[k - 1], h_recv.at[k - 1],
            device_id=(b, other), device_id_type=MESH,
        )
        copy.start()
        half_copies.append(copy)

    def column_copy(k):
        to = (b + far_first(k, nb)) % nb
        return pltpu.make_async_remote_copy(
            dens.at[:, to], dcol.at[b], d_send.at[k], d_recv.at[k],
            device_id=(to, s), device_id_type=MESH,
        )

    loop(0, nb - 1, lambda k: column_copy(k).start())
    dcol[b] = dens[:, b]

    nbl = occupation.shape[1]
    depth = rows * nbl
    band = lax.broadcasted_iota(jnp.int32, (depth, 128), 0) % nbl
    weight = jnp.zeros((depth, 128), jnp.float32)
    for j in range(nbl):
        share = jnp.full((depth, 128), occupation[0, j]).astype(jnp.float32) / occupation_unit
        weight = jnp.where(band == j, share, weight)
    for fetch in fetches[1:3]:
        fetch.wait()

    def kinetic(i):
        here = pl.ds(pl.multiple_of(i * depth, depth), depth)
        real, imag = coef[0, here, :].astype(jnp.float32), coef[1, here, :].astype(jnp.float32)
        high, low = split(weight * (real * real + imag * imag))
        kin[i // (2 * ns), (i // ns) % 2, i % ns] = jnp.dot(
            pairs[...], high, preferred_element_type=jnp.float32
        ) + jnp.dot(pairs[...], low, preferred_element_type=jnp.float32)

    loop(0, n, kinetic)
    core_copy = pltpu.make_async_remote_copy(
        kin.at[:, 1 - core], from_core, c_send.at[0], c_recv.at[0],
        device_id=(b + 1 - 2 * core, s), device_id_type=MESH,
    )
    core_copy.start()
    for copy in half_copies:
        copy.wait()
    for fetch in fetches[3:5]:
        fetch.wait()

    def plane(i):
        total = dens[s * zh + i]
        for k in range(ns - 1):
            total = total + half[k, i]
        along = dot3((table_x[0], table_x[1]), split(total.reshape(nx, width)))
        both = split(jnp.concatenate([along[:nx], along[nx:]], axis=1))
        for k in range(ns):
            spec[k, i] = dot3(both, (table_y[0, k], table_y[1, k])).reshape(nb, xl, -1)

    loop(0, zh, plane)

    def spec_copy(k):
        offset = far_first(k, n)
        tb, ts = (b + offset // ns) % nb, (s + offset % ns) % ns
        return pltpu.make_async_remote_copy(
            spec.at[ts, :, tb], scol.at[b, s], s_send.at[k], s_recv.at[k],
            device_id=(tb, ts), device_id_type=MESH,
        )

    loop(0, n - 1, lambda k: spec_copy(k).start())
    scol[b, s] = spec[s, :, b]

    core_copy.wait()

    def add_core(i):
        sum_core[i // ny, i % ny] = kin[i, core] + from_core[i]

    loop(0, nz * ny, add_core)
    plane_copies = []
    for k in range(1, ny * ns):
        ty, ts = (y + k // ns) % ny, (s + k % ns) % ns
        copy = pltpu.make_async_remote_copy(
            sum_core.at[:, ty, ts], from_plane.at[k - 1], p_send.at[k - 1], p_recv.at[k - 1],
            device_id=((z * ny + ty) * 2 + core, ts), device_id_type=MESH,
        )
        copy.start()
        plane_copies.append(copy)

    fetches[5].wait()

    def in_plane(i):
        value = split(dens[i].reshape(nx, width))
        grad_x[i] = dot3((table_g[0, 0], table_g[1, 0]), value)
        grad_y[i] = dot3(value, (table_g[0, 1], table_g[1, 1]))

    loop(0, zl, in_plane)

    fetches[6].wait()
    loop(0, nb - 1, lambda k: column_copy(k).wait())
    for x in range(xl):
        column = split(dcol[:, :, x, :].reshape(nb * zl, width))
        grad[:, :, x, :] = dot3((table_d[0], table_d[1]), column).reshape(nb, zl, width)

    def grad_copy(k):
        to = (b + far_first(k, nb)) % nb
        return pltpu.make_async_remote_copy(
            grad.at[to], gout.at[:, b], g_send.at[k], g_recv.at[k],
            device_id=(to, s), device_id_type=MESH,
        )

    loop(0, nb - 1, lambda k: grad_copy(k).start())
    gout[:, b] = grad[b]

    for copy in plane_copies:
        copy.wait()
    total = sum_core[:, y, s]
    for k in range(1, ny * ns):
        total = total + from_plane[k - 1]
    sum_plane[...] = total

    def line_copy(k):
        tz = (z + k) % nz
        return pltpu.make_async_remote_copy(
            sum_plane.at[tz], from_line.at[k - 1], l_send.at[k - 1], l_recv.at[k - 1],
            device_id=((tz * ny + y) * 2 + core, s), device_id_type=MESH,
        )

    loop(1, nz, lambda k: line_copy(k).start())
    loop(1, nz, lambda k: line_copy(k).wait())
    kweight = sum_plane[z] + jnp.sum(from_line[...], axis=0)
    gk = [spacing * (miller[i].astype(jnp.float32) + kpoint[i]) for i in range(3)]
    kdens[...] = 0.5 * (gk[0] * gk[0] + gk[1] * gk[1] + gk[2] * gk[2]) * kweight
    scaled = kweight * (-1.0 / (n * rows * 128))
    order = ((0, 0), (1, 1), (2, 2), (1, 2), (0, 2), (0, 1))
    part[...] = jnp.zeros_like(part)
    for i, (p, q) in enumerate(order):
        part[pl.ds(i, 1), :] = fold(scaled * gk[p] * gk[q])

    loop(0, n - 1, lambda k: spec_copy(k).wait())
    for fetch in fetches[7:]:
        fetch.wait()
    lanes = scol.shape[4]
    count = lanes // 2
    lane = lax.broadcasted_iota(jnp.int32, (nzg, lanes), 1)
    first = lane < count
    freq_z = axis_frequency(lax.broadcasted_iota(jnp.int32, (nzg, lanes), 0), nzg)
    freq_y = axis_frequency(lane % count + s * count, width)
    row_y = freq_y[:1]
    share = lane * 0 + s
    for x in range(xl):
        column = split(scol[:, :, :, x, :].reshape(nzg, lanes))
        turned = dot3((table_z[0], table_z[1]), column)
        swapped = pltpu.roll(turned[nzg:], count, 1)
        value = turned[:nzg] + jnp.where(first, swapped, -swapped)
        local = jnp.zeros_like(value)
        for k in range(ns):
            left, right = factor[0, :, x, :], factor[1, :, x, :]
            if k > 0:
                left = pltpu.roll(left, width - k * count, 1)
            if k != 1:
                right = pltpu.roll(right, (width - k * count + count) % width, 1)
            local = jnp.where(share == k, jnp.where(first, left, right), local)
        position = jnp.full((nzg, lanes), b * xl + x)
        freq_x = axis_frequency(position, nx)
        length = freq_x * freq_x + freq_y * freq_y + freq_z * freq_z
        positive = length > 0
        inverse = jnp.where(positive, 1.0 / jnp.where(positive, length, 1.0), 0.0)
        hartree = 4.0 * np.pi * value * value * inverse
        weigh = 2.0 * (hartree * inverse + value * local)
        weigh_z = weigh * freq_z
        plain, along_z, along_zz = fold(weigh), fold(weigh_z), fold(weigh_z * freq_z)
        trace = fold(hartree)
        row_x = freq_x[:1]
        terms = (
            plain * row_x * row_x - trace,
            plain * row_y * row_y - trace,
            along_zz - trace,
            along_z * row_y,
            along_z * row_x,
            plain * row_x * row_y,
        )
        for i, term in enumerate(terms):
            part[pl.ds(i, 1), :] += term

    loop(0, nb - 1, lambda k: grad_copy(k).wait())

    def exchange(i):
        value = dens[i].reshape(nx, width)
        g = (grad_x[i], grad_y[i], gout[i].reshape(nx, width))
        total = g[0] * g[0] + g[1] * g[1] + g[2] * g[2]
        square[i] = total
        scale = 4.0 * value * value + 1.0
        weigh = jnp.exp(jnp.log(value) * (-1.0 / 3.0)) * scale / (scale + total)
        weigh = weigh * (-1.0 / (nzg * nx * width))
        for j, (p, q) in enumerate(order):
            part[pl.ds(j, 1), :] += fold(weigh * g[p] * g[q])

    loop(0, zl, exchange)

    def stress_copy(k):
        tb, ts = (b + k // ns) % nb, (s + k % ns) % ns
        return pltpu.make_async_remote_copy(
            part, held.at[k - 1], t_send.at[k - 1], t_recv.at[k - 1],
            device_id=(tb, ts), device_id_type=MESH,
        )

    loop(1, n, lambda k: stress_copy(k).start())
    loop(1, n, lambda k: stress_copy(k).wait())
    stress[...] = part[...] + jnp.sum(held[...], axis=0)


def params(number):
    return pltpu.CompilerParams(
        collective_id=number, has_side_effects=True, vmem_limit_bytes=60 * 2**20
    )


def f32(*shape):
    return jax.ShapeDtypeStruct(shape, jnp.float32)


def shards(nb, ns, coefficients, occupation, miller, density, local_factor):
    dma = pltpu.SemaphoreType.DMA
    _, zl, nx, ny = density.shape
    nzg = zl * nb
    xl = nx // nb
    zh = zl // ns
    part = ny // ns
    lanes = 2 * part
    npw = coefficients.shape[3]
    rows = npw // (nb * ns * 128)
    nbl = coefficients.shape[2]
    fold_y = 2 if nb % 4 == 0 else 1
    fold_z = nb // (2 * fold_y)

    coef = coefficients[0].reshape(2, nbl, npw // 128, 128)
    coef = coef.transpose(0, 2, 1, 3).reshape(2, npw // 128 * nbl, 128)
    pairs = jnp.asarray(np.kron(np.eye(rows), np.ones((1, nbl))), jnp.bfloat16)
    cos_x, sin_x = fourier_tables(nx)
    cos_y, sin_y = fourier_tables(ny)
    cos_z, sin_z = fourier_tables(nzg)
    table_y = []
    for k in range(ns):
        cut = slice(k * part, (k + 1) * part)
        table_y.append(np.block([[cos_y[:, cut], -sin_y[:, cut]], [sin_y[:, cut], cos_y[:, cut]]]))
    in_plane = [derivative_table(nx).astype(np.float64), derivative_table(ny).T.astype(np.float64)]
    fetched = (
        density[0].reshape(zl, nb, xl, ny),
        coef,
        local_factor,
        host_split(np.concatenate([cos_x, -sin_x])),
        host_split(np.stack(table_y)),
        host_split(derivative_table(nzg).astype(np.float64)),
        host_split(np.concatenate([cos_z, sin_z]) / (nzg * nx * ny)),
        host_split(np.stack(in_plane)),
        pairs,
    )

    stress, kinetic_density, square = pl.pallas_call(
        functools.partial(main_kernel, nb, ns, fold_y, fold_z),
        out_shape=(f32(8, 128), f32(rows, 128), f32(zl, nx, ny)),
        in_specs=[pl.BlockSpec(memory_space=pltpu.SMEM), VMEM]
        + [pl.BlockSpec(memory_space=pltpu.HBM)] * len(fetched),
        out_specs=(VMEM,) * 3,
        scratch_shapes=[pltpu.VMEM(value.shape, value.dtype) for value in fetched]
        + [
            pltpu.VMEM(shape, jnp.float32)
            for shape in (
                (fold_z * fold_y, 2, ns, rows, 128),
                (nb, zl, xl, ny),
                (ns - 1, zh, nb, xl, ny),
                (ns, zh, nb, xl, lanes),
                (nb, zl, xl, ny),
                (fold_z * fold_y, ns, rows, 128),
                (fold_z, fold_y, ns, rows, 128),
                (fold_y * ns - 1, fold_z, rows, 128),
                (fold_z, rows, 128),
                (fold_z - 1, rows, 128),
                (nb, ns, zh, xl, lanes),
                (zl, nb, xl, ny),
                (zl, nx, ny),
                (zl, nx, ny),
                (8, 128),
                (nb * ns - 1, 8, 128),
            )
        ]
        + [dma((len(fetched),))]
        + [
            dma((count,))
            for length in (
                nb - 1, ns - 1, 1, fold_y * ns - 1, fold_z - 1, nb * ns - 1, nb - 1, nb * ns - 1,
            )
            for count in (length, length)
        ],
        compiler_params=params(0),
        name="main_exchange",
    )(occupation, miller.reshape(3, rows, 128), *fetched)
    return (
        jnp.sum(stress[:6], axis=1),
        kinetic_density.reshape(rows * 128),
        square[None],
    )


def solution(mesh):
    return jax.shard_map(
        functools.partial(shards, mesh.shape["band"], mesh.shape["spin"]),
        mesh=mesh,
        in_specs=(
            P("spin", None, "band", None),
            P("spin", "band"),
            P(None, ("band", "spin")),
            P("spin", "band", None, None),
            P(None, None, "band", None),
        ),
        out_specs=(P(), P(("band", "spin")), P("spin", "band", None, None)),
        check_vma=False,
    )
```
